32 devices in a mesh: row: 8 (over z, x), col: 4 (over y, core), ga: 1.
Axes of the slice: x: 2, y: 2, z: 4, core: 2. Of those that a mesh axis runs over, the one named last changes fastest.
Arguments:
- pair_density: float32 [512, 24, 3072], P('row', None, 'ga'), may hold values from -6 to 6
- coulomb: float32 [3072], P('ga'), may hold values from 0.1 to 2
Outputs:
- kernel: float32 [12288, 12288], P('row', 'col')
The draws below stay inside these ranges and needn't reach their ends.
All inputs are finite; a program needn't handle non-finite values.
Results may differ from the reference program's by a relative error of at most 0.00011.
Values sent between devices are 32-bit elements; how exact they have to be, the bound alone decides.
A program may use at most 192 MiB of HBM per device.

```python
import math
import jax
import jax.numpy as jnp
from jax import lax

NG = 3072
NK = 512
NVC = 24
N_ROW = 8
N_COL = 4


def level_of(own_key, extent, cuts, low, top_value):
    gain, own = 1.0, jax.random.fold_in(own_key, 6)
    for position, blocks in cuts:
        steps = jnp.exp(jax.random.uniform(jax.random.fold_in(own, position), (blocks,), jnp.float32, low / len(cuts), top_value / len(cuts)))
        gain = gain * jnp.repeat(steps, extent[position] // blocks).reshape([-1 if axis == position else 1 for axis in range(len(extent))])
    return gain


def bell_draw(rng, shape, spread, limit, split=(), kind=jnp.bfloat16):
    drawn = spread * jax.random.normal(rng, shape, jnp.float32)
    if split:
        drawn = drawn * level_of(rng, shape, split, -0.22, 0.18)
    return jnp.clip(drawn, -limit, limit).astype(kind)


def setup_inputs(seed: int = 0) -> dict:
    key_of = jax.random.split(jax.random.key(seed), 3)
    pair_density = bell_draw(key_of[0], (NK, NVC, NG), 1.0, 6.0, ((0, 8),), jnp.float32)
    coulomb = jnp.clip(jnp.exp(jax.random.uniform(key_of[1], (NG,), jnp.float32, math.log(0.1), math.log(2.0))), 0.1, 2.0)
    return {"pair_density": pair_density, "coulomb": coulomb}


def contract(left_rows, right_rows):
    return lax.dot_general(left_rows, right_rows, (((1,), (1,)), ((), ())), precision=lax.Precision.HIGHEST, preferred_element_type=jnp.float32)


def reference(pair_density, coulomb):
    row_order = jnp.arange(NK, dtype=jnp.int32).reshape(NK // N_ROW, N_ROW).T.reshape(-1)
    col_order = jnp.arange(NK, dtype=jnp.int32).reshape(NK // N_COL, N_COL).T.reshape(-1)
    left = pair_density[row_order]
    right = pair_density[col_order]
    bands = pair_density.shape[1]
    g_width = pair_density.shape[2]
    weighted = left.reshape(NK * bands, g_width) * (2.0 * coulomb)[None, :]
    exchange = contract(weighted, right.reshape(NK * bands, g_width))
    return exchange / jnp.float32(NK)
```

```python
import functools

import jax
import jax.numpy as jnp
from jax import lax
from jax.sharding import PartitionSpec as P

LANES = 128
SHARES = (4, 4, 4, 4, 4, 2, 2)


def contract(left_rows, right_rows):
    return lax.dot_general(
        left_rows,
        right_rows,
        (((1,), (1,)), ((), ())),
        precision=lax.Precision.HIGH,
        preferred_element_type=jnp.float32,
    )


def widths_of(total):
    units, shares = total // LANES, sum(SHARES)
    cuts, seen = [0], 0
    for share in SHARES:
        seen += share
        cuts.append(units * seen // shares * LANES)
    cuts[-1] = total
    return [(a, b) for a, b in zip(cuts, cuts[1:]) if b > a]


def spread(rows, row_count, col_count):
    here_row, here_col = lax.axis_index("row"), lax.axis_index("col")
    away = jnp.bitwise_xor(here_col, here_row % col_count)
    bit = col_count // 2
    while bit:
        pairs = []
        for r in range(row_count):
            for c in range(col_count):
                if (c ^ (r % col_count)) % (2 * bit) == 0:
                    pairs.append((r * col_count + c, r * col_count + (c ^ bit)))
        got = lax.ppermute(rows, ("row", "col"), pairs)
        rows = jnp.where(away % (2 * bit) == bit, got, rows)
        bit //= 2
    return rows


def local(pair_density, coulomb):
    row_count = lax.axis_size("row")
    col_count = lax.axis_size("col")
    here_row = lax.axis_index("row")
    here_col = lax.axis_index("col")
    local_k, bands, g_width = pair_density.shape
    total_k = local_k * row_count
    scale = (2.0 * coulomb) / jnp.float32(total_k)
    grouped = pair_density.reshape(local_k // col_count, col_count, bands, g_width)
    ratio = row_count // col_count
    total = None
    for start, stop in widths_of(g_width):
        width = stop - start
        own = lax.dynamic_slice(
            grouped, (0, here_col, 0, start), (local_k // col_count, 1, bands, width)
        )[:, 0]
        piece = lax.all_gather(own, "row", axis=0, tiled=True)
        paired = piece.reshape(piece.shape[0] // ratio, ratio, bands, width)
        rows = lax.dynamic_index_in_dim(paired, here_row // col_count, 1, keepdims=False)
        rows = spread(rows, row_count, col_count)
        weighted = rows.reshape(local_k * bands, width) * scale[None, start:stop]
        part = contract(weighted, piece.reshape(piece.shape[0] * bands, width))
        total = part if total is None else total + part
    return lax.psum(total, "ga")


def solution(mesh):
    placed = (P("row", None, "ga"), P("ga"))
    return jax.shard_map(
        local, mesh=mesh, in_specs=placed, out_specs=P("row", "col"), check_vma=False
    )
```
